32 devices in a mesh: node: 8 (over z, x), local: 4 (over y, core).
Axes of the slice: x: 2, y: 2, z: 4, core: 2. Of those that a mesh axis runs over, the one named last changes fastest.
Arguments:
- hidden: bfloat16 [8, 64, 16384], P('node'), may hold values from -6 to 6
- down_weight: bfloat16 [131072, 6144], P('node', 'local'), may hold values from -0.046875 to 0.046875
- expert_ids: int32 [128, 2], P(('node', 'local')), may hold values from 0 to 7, all different within a row; in each aligned block of 4 rows (0 to 3, 4 to 7, ...) at most 2 rows name the same one
- gate_logits: float32 [128, 2], P(('node', 'local')), may hold values from -6 to 6
- residual: bfloat16 [128, 6144], P(('node', 'local')), may hold values from -6 to 6
Outputs:
- mixed: bfloat16 [128, 6144], P(('node', 'local'))
The draws below stay inside these ranges and needn't reach their ends.
Inputs may be any that keep to these rules, and one draw needn't show every extreme that they name: `expert_ids`: each row names 2 different experts. The 4 tokens of one device name one expert at most 2 times, and some device names some expert exactly 2 times.
All inputs are finite; a program needn't handle non-finite values.
Results may differ from the reference program's by a relative error of at most 0.006.
Values may be sent and summed in bfloat16 or wider, within the bound.
A program may use at most 128 MiB of HBM per device.

```python
import math
import jax
import jax.numpy as jnp
import numpy as np
from jax import lax

D = 6144
FF = 16384
EXPERTS = 8
TOP = 2
TOK_DEV = 4
FF_NODE = 16384
CAP = 2
SLOTS = 64
TOKENS = 128
N_NODE = 8
N_LOCAL = 4


def steps_of(rng, extent, split, least, high):
    level = 1.0
    for position, shards_of in split:
        heights = jax.random.uniform(jax.random.fold_in(jax.random.fold_in(rng, 6), position), (shards_of,), jnp.float32, least / len(split), high / len(split))
        level = level * jnp.repeat(jnp.exp(heights), extent[position] // shards_of).reshape((-1,) + (1,) * (len(extent) - 1 - position))
    return level


def deal_out(own_key, own, number, rows, count, top, limit, slope):
    order = jax.random.permutation(own_key, count)
    heavy_load, ordinary = shares(count, rows * top, limit, slope, True), shares(count, rows * top, limit, slope, False)
    places = jnp.arange(count)

    def named(lengths, turn):
        used = int((lengths > 0).sum())
        fixed = max(1, used // 4)
        shifted = fixed + (places - fixed + turn * (used - fixed)) % max(1, count - fixed)
        return jnp.zeros((count,), jnp.int32).at[order[jnp.where(places < fixed, places, shifted)]].set(jnp.asarray(lengths, jnp.int32))

    lengths = jnp.where(number % 4 == 0, named(heavy_load, number // 4), named(ordinary, number - number // 4 - 1))
    mixed = jax.random.permutation(jax.random.fold_in(own, 3), count)
    donor, receiver = mixed[0:count // 2 * 2:2], mixed[1:count // 2 * 2:2]
    slack = jnp.minimum(lengths[donor] - 1, limit - lengths[receiver]) // 2
    slack = jnp.where((donor == order[0]) | (receiver == order[0]) | (lengths[receiver] == 0), 0, jnp.maximum(slack, 0))
    shifted = jax.random.randint(jax.random.fold_in(own, 4), (count // 2,), 0, 1 << 20) % (slack + 1)
    lengths = lengths.at[donor].add(-shifted).at[receiver].add(shifted)
    items = jnp.searchsorted(jnp.cumsum(lengths), jnp.arange(rows * top), side="right").astype(jnp.int32)
    table = items.reshape(top, rows).T
    table = table[jax.random.permutation(jax.random.fold_in(own, 1), rows)]
    turn = jax.random.randint(jax.random.fold_in(own, 2), (rows, 1), 0, top)
    return jnp.take_along_axis(table, (jnp.arange(top)[None, :] + turn) % top, axis=1)


def shares(amount, total, limit, skew, full):
    weights = [(1 << 20) // math.isqrt(rank ** skew) + 1 for rank in range(1, amount + 1)]
    largest = limit if full else min(limit, max(-(-total // amount), total * weights[0] // sum(weights)))
    least = 1 if total - largest >= amount - 1 else 0
    holding, surplus = [largest] + [least] * (amount - 1), total - largest - least * (amount - 1)
    while surplus > 0:
        movable = [i for i in range(1, amount) if holding[i] < largest] or [i for i in range(1, amount) if holding[i] < limit]
        pool, remaining = sum([weights[i] for i in movable]), surplus
        for i in movable:
            addition = min(limit - holding[i], max(1, remaining * weights[i] // pool), surplus)
            holding[i] = holding[i] + addition
            surplus = surplus - addition
    return np.array(holding)


def centred(own_key, shape, scale, most, cuts=(), kind=jnp.bfloat16):
    array = scale * jax.random.normal(own_key, shape, jnp.float32)
    if cuts:
        array = array * steps_of(own_key, shape, cuts, -0.22, 0.18)
    return jnp.clip(array, -most, most).astype(kind)


def setup_inputs(seed: int = 0) -> dict:
    key_list = jax.random.split(jax.random.key(seed), 6)
    hidden = centred(key_list[0], (N_NODE, SLOTS, FF_NODE), 1.0, 6.0, ((0, 8),))
    down_weight = centred(key_list[1], (EXPERTS * FF, D), FF ** -0.5, 0.046875, ((0, 8), (1, 4)))
    expert_ids_keys = jax.random.split(jax.random.fold_in(key_list[2], 1), TOKENS // TOK_DEV)
    expert_ids_turns = jax.random.permutation(jax.random.fold_in(key_list[2], 3), TOKENS // TOK_DEV)
    expert_ids = jax.vmap(lambda own, number: deal_out(jax.random.fold_in(key_list[2], 2), own, number, TOK_DEV, EXPERTS, TOP, CAP, 2))(expert_ids_keys, expert_ids_turns).reshape((TOKENS, TOP))
    gate_logits = centred(key_list[3], (TOKENS, TOP), 1.5, 6.0, ((0, 32),), jnp.float32)
    residual = centred(key_list[4], (TOKENS, D), 1.0, 6.0, ((0, 32),))
    return dict(hidden=hidden, down_weight=down_weight, expert_ids=expert_ids, gate_logits=gate_logits, residual=residual)


def tree_total(stacked):
    values = stacked
    while values.shape[0] > 1:
        half_size = values.shape[0] // 2
        values = (values[:half_size].astype(jnp.float32) + values[half_size:].astype(jnp.float32)).astype(jnp.bfloat16)
    return values[0]


def gate_pair(gate_logits):
    first_gate = 1.0 / (1.0 + jnp.exp(gate_logits[:, 1] - gate_logits[:, 0]))
    second = 1.0 / (1.0 + jnp.exp(gate_logits[:, 0] - gate_logits[:, 1]))
    return jnp.stack([first_gate, second], axis=1)


def slot_numbers(expert_ids, owners_count, per_owner):
    onehot = (expert_ids[:, :, None] == jnp.arange(EXPERTS, dtype=jnp.int32)[None, None, :]).astype(jnp.int32)
    counts = jnp.sum(onehot, axis=1).reshape(owners_count, per_owner, EXPERTS)
    before = (jnp.cumsum(counts, axis=1) - counts).reshape(owners_count * per_owner, EXPERTS)
    return jnp.sum(before[:, None, :] * onehot, axis=2).astype(jnp.int32)


def reference(hidden, down_weight, expert_ids, gate_logits, residual):
    shards = N_NODE // EXPERTS
    ffn_node = FF // shards
    owners_count = N_NODE * N_LOCAL
    gate_values = gate_pair(gate_logits.astype(jnp.float32))
    slot_of = slot_numbers(expert_ids, owners_count, TOK_DEV)
    owner_dev = (jnp.arange(owners_count * TOK_DEV, dtype=jnp.int32) // TOK_DEV).astype(jnp.int32)
    row_index = (owner_dev[:, None] * CAP + slot_of).astype(jnp.int32)

    def one_expert(running, expert):
        inputs = lax.dynamic_slice_in_dim(hidden, expert * shards, shards, 0)
        weights = lax.dynamic_slice_in_dim(down_weight, expert * (shards * ffn_node), shards * ffn_node, 0)
        shard_terms = []
        for shard_no in range(shards):
            weight_rows = weights[shard_no * ffn_node:(shard_no + 1) * ffn_node]
            shard_terms.append(jnp.dot(inputs[shard_no], weight_rows, preferred_element_type=jnp.float32).astype(jnp.bfloat16))
        expert_rows = tree_total(jnp.stack(shard_terms))
        for member in range(TOP):
            picked = expert_rows[row_index[:, member]].astype(jnp.float32)
            chosen = expert_ids[:, member] == expert
            running = running + jnp.where(chosen[:, None], gate_values[:, member, None] * picked, 0.0)
        return running, None

    zero_total = jnp.zeros((owners_count * TOK_DEV, D), jnp.float32)
    running, unused = lax.scan(one_expert, zero_total, jnp.arange(EXPERTS, dtype=jnp.int32))
    return (residual.astype(jnp.float32) + running).astype(jnp.bfloat16)
```

```python
import functools

import jax
import jax.numpy as jnp
from jax import lax
from jax.experimental import pallas as pl
from jax.experimental.pallas import tpu as pltpu
from jax.sharding import PartitionSpec as P

EXPERTS = 8
DEPTH = 2048
AHEAD = 3
VMEM = 56 << 20
UNROLL = lambda n: n - 1 if n <= 32 else 1
ROWS = 64
MESH = pl.DeviceIdType.MESH


def block_list(width):
    last = min(256, width)
    rest = width - last
    middle = min(512, rest // 256 * 256)
    sizes = [size for size in (rest - middle, middle, last) if size]
    return [(sum(sizes[:i]), size) for i, size in enumerate(sizes)]


def tree_total(values):
    while len(values) > 1:
        half = len(values) // 2
        values = [
            (values[i].astype(jnp.float32) + values[i + half].astype(jnp.float32)).astype(
                jnp.bfloat16
            )
            for i in range(half)
        ]
    return values[0]


def selector_of(ids, logits, capacity):
    tokens = ids.shape[1]
    first, second = logits[0:1, :], logits[1:2, :]
    gates = (1.0 / (1.0 + jnp.exp(second - first)), 1.0 / (1.0 + jnp.exp(first - second)))
    shape = (EXPERTS * capacity, tokens)
    row = lax.broadcasted_iota(jnp.int32, shape, 0)
    token = lax.broadcasted_iota(jnp.int32, shape, 1)
    expert, place = row // capacity, row % capacity
    match = [ids[k : k + 1, :] == expert for k in range(2)]
    count = match[0].astype(jnp.int32) + match[1].astype(jnp.int32)
    before = jnp.zeros(shape, jnp.int32)
    for t in range(tokens - 1):
        before = before + jnp.where(token > t, count[:, t : t + 1], 0)
    here = before == place
    return sum(jnp.where(match[k] & here, gates[k], 0.0) for k in range(2)).T


def kernel(
    nodes, locals_, h_hbm, w_hbm, ids_hbm, logits_hbm, res_hbm, out_ref,
    h, w, acc, send, recv, ids, logits, res, h_sem, w_sem, small_sem, send_sem, recv_sem,
):
    owners = nodes * locals_
    rows, inner = h.shape
    width = w.shape[1]
    capacity = rows // owners
    depth = min(DEPTH, inner)
    steps = inner // depth
    blocks = block_list(width)
    shards = nodes // EXPERTS
    tokens = ids.shape[1]
    my_node, my_local = lax.axis_index("node"), lax.axis_index("local")
    me = my_node * locals_ + my_local

    def h_copy(k):
        part = pl.ds(k * depth, depth)
        return pltpu.make_async_copy(h_hbm.at[0, :, part], h.at[:, part], h_sem.at[k])

    def w_copy(b, k):
        first, size = blocks[b]
        at = (pl.ds(k * depth, depth), pl.ds(first, size))
        return pltpu.make_async_copy(w_hbm.at[at], w.at[at], w_sem.at[b, k])

    smalls = [
        pltpu.make_async_copy(src, dst, small_sem.at[i])
        for i, (src, dst) in enumerate([(ids_hbm, ids), (logits_hbm, logits), (res_hbm, res)])
    ]
    order = [(b, k) for b in range(len(blocks)) for k in range(steps)]

    def start(place):
        if place < len(order):
            b, k = order[place]
            if b == 0:
                h_copy(k).start()
            w_copy(b, k).start()

    for place in range(AHEAD):
        start(place)
    for copy in smalls:
        copy.start()

    def peer(i):
        turn = (i + 1) // 2
        other = lax.rem(me + owners // 2 + jnp.where(i % 2 == 1, turn, -turn) + owners, owners)
        return other, (other // locals_, lax.rem(other, locals_))

    barrier = pltpu.get_barrier_semaphore()

    @pl.loop(0, owners - 1)
    def _(i):
        pl.semaphore_signal(barrier, inc=1, device_id=peer(i)[1], device_id_type=MESH)

    per_tile = ROWS // capacity
    for b, (first, size) in enumerate(blocks):
        columns = pl.ds(first, size)
        for k in range(steps):
            if b == 0:
                h_copy(k).wait()
            w_copy(b, k).wait()
            start(b * steps + k + AHEAD)
            part = pl.ds(k * depth, depth)

            @pl.loop(0, rows // ROWS)
            def _(m):
                at = pl.ds(pl.multiple_of(m * ROWS, ROWS), ROWS)
                term = jnp.dot(h[at, part], w[part, columns], preferred_element_type=jnp.float32)
                if k > 0:
                    term = acc[at, pl.ds(0, size)] + term
                if k < steps - 1:
                    acc[at, pl.ds(0, size)] = term
                else:
                    send[pl.ds(m * per_tile, per_tile), :, columns] = term.astype(
                        jnp.bfloat16
                    ).reshape(per_tile, capacity, size)

        if b == 0:
            pl.semaphore_wait(barrier, owners - 1)
        landing = pl.ds(pl.multiple_of(my_local * width + first, 128), size)

        @pl.loop(0, owners - 1, unroll=UNROLL(owners))
        def _(i):
            other, device = peer(i)
            pltpu.make_async_remote_copy(
                src_ref=send.at[other, :, columns],
                dst_ref=recv.at[my_node, :, landing],
                send_sem=send_sem,
                recv_sem=recv_sem.at[b],
                device_id=device,
                device_id_type=MESH,
            ).start()

        pltpu.make_async_copy(
            send.at[me, :, columns], recv.at[my_node, :, landing], recv_sem.at[b]
        ).start()

    for copy in smalls:
        copy.wait()
    selector = selector_of(ids[...], logits[...], capacity)
    padded = -(-tokens // 8) * 8
    if padded > tokens:
        selector = jnp.concatenate(
            [selector, jnp.zeros((padded - tokens, selector.shape[1]), jnp.float32)], axis=0
        )
    high = selector.astype(jnp.bfloat16).astype(jnp.float32)
    middle = (selector - high).astype(jnp.bfloat16).astype(jnp.float32)
    low = selector - high - middle
    terms = jnp.concatenate([high, middle, low], axis=0).astype(jnp.bfloat16)

    for b, (first, size) in enumerate(blocks):
        whole = recv.at[:, :, pl.ds(0, locals_ * size)]
        pltpu.make_async_copy(whole, whole, recv_sem.at[b]).wait()

        for part in range(locals_):
            columns = pl.ds(part * width + first, size)
            got = recv[:, :, columns].reshape(EXPERTS, shards, capacity, size)
            picked = tree_total([got[:, s] for s in range(shards)])
            picked = picked.reshape(EXPERTS * capacity, size)
            sums = jnp.dot(terms, picked, preferred_element_type=jnp.float32)
            total = sums[:padded] + sums[padded : 2 * padded] + sums[2 * padded :]
            out_ref[:, columns] = (res[:, columns].astype(jnp.float32) + total[:tokens]).astype(
                jnp.bfloat16
            )

    sent = send.at[pl.ds(0, owners - 1)]
    pltpu.make_async_copy(sent, sent, send_sem).wait()


def local(hidden, down_weight, expert_ids, gate_logits, residual):
    nodes, locals_ = lax.axis_size("node"), lax.axis_size("local")
    owners = nodes * locals_
    rows, inner = hidden.shape[1:]
    width = down_weight.shape[1]
    capacity = rows // owners
    blocks = block_list(width)
    steps = inner // min(DEPTH, inner)
    widest = max(size for _, size in blocks)
    scratch = [
        pltpu.VMEM((rows, inner), jnp.bfloat16),
        pltpu.VMEM((inner, width), jnp.bfloat16),
        pltpu.VMEM((rows, widest), jnp.float32),
        pltpu.VMEM((owners, capacity, width), jnp.bfloat16),
        pltpu.VMEM((nodes, capacity, residual.shape[1]), jnp.bfloat16),
        pltpu.VMEM(expert_ids.shape[::-1], jnp.int32),
        pltpu.VMEM(gate_logits.shape[::-1], jnp.float32),
        pltpu.VMEM(residual.shape, jnp.bfloat16),
        pltpu.SemaphoreType.DMA((steps,)),
        pltpu.SemaphoreType.DMA((len(blocks), steps)),
        pltpu.SemaphoreType.DMA((3,)),
        pltpu.SemaphoreType.DMA,
        pltpu.SemaphoreType.DMA((len(blocks),)),
    ]
    return pl.pallas_call(
        functools.partial(kernel, nodes, locals_),
        out_shape=jax.ShapeDtypeStruct(residual.shape, jnp.bfloat16),
        in_specs=[pl.BlockSpec(memory_space=pltpu.HBM)] * 5,
        out_specs=pl.BlockSpec(memory_space=pltpu.VMEM),
        scratch_shapes=scratch,
        compiler_params=pltpu.CompilerParams(collective_id=0, has_side_effects=True, vmem_limit_bytes=VMEM),
    )(hidden, down_weight, expert_ids.T, gate_logits.T, residual)


def solution(mesh):
    return jax.shard_map(
        local,
        mesh=mesh,
        in_specs=(
            P("node", None, None),
            P("node", "local"),
            P(("node", "local"), None),
            P(("node", "local"), None),
            P(("node", "local"), None),
        ),
        out_specs=P(("node", "local"), None),
        check_vma=False,
    )
```
